32 devices in a mesh: rep: 2 (over x), dp: 16 (over y, z, core).
Axes of the slice: x: 2, y: 2, z: 4, core: 2. Of those that a mesh axis runs over, the one named last changes fastest.
Arguments:
- x: bfloat16 [32, 2048, 640], P(('rep', 'dp')), parts along dimension 0
- dy: bfloat16 [32, 2048, 640], P(('rep', 'dp')), parts along dimension 0
- w_gate: bfloat16 [2, 640, 2048], replicated
- w_up: bfloat16 [2, 640, 2048], replicated
- w_down: bfloat16 [2, 2048, 640], replicated
- m_w_gate: float32 [2, 640, 2048], replicated
- m_w_up: float32 [2, 640, 2048], replicated
- m_w_down: float32 [2, 2048, 640], replicated
- v_w_gate: float32 [2, 640, 2048], replicated
- v_w_up: float32 [2, 640, 2048], replicated
- v_w_down: float32 [2, 2048, 640], replicated
Outputs:
- output 1: bfloat16 [4, 640, 2048], P('rep'), parts along dimension 0
- output 2: bfloat16 [4, 640, 2048], P('rep'), parts along dimension 0
- output 3: bfloat16 [4, 2048, 640], P('rep'), parts along dimension 0
- output 4: float32 [4, 640, 2048], P('rep'), parts along dimension 0
- output 5: float32 [4, 640, 2048], P('rep'), parts along dimension 0
- output 6: float32 [4, 2048, 640], P('rep'), parts along dimension 0
- output 7: float32 [4, 640, 2048], P('rep'), parts along dimension 0
- output 8: float32 [4, 640, 2048], P('rep'), parts along dimension 0
- output 9: float32 [4, 2048, 640], P('rep'), parts along dimension 0
There are 2 independent parts. The reference program is written for one: setup_inputs(seed, part) draws one part's arguments, and reference() takes and returns one part's arrays. A program takes and returns all parts, laid end to end along the dimension named above; an argument that names none is the same for every part.
All inputs are finite; a program needn't handle non-finite values.
Results may differ from the reference program's by a relative error of at most 0.022.
Values are sent between devices in bfloat16 or wider.
A program may use at most 2.25 GiB of HBM per device.

```python
import jax
import jax.numpy as jnp
from jax import lax

SEQUENCES = 16
TOKENS = 2048
D = 640
FF = 2048
LAYERS = 2
NAMES = ("w_gate", "w_up", "w_down")
SHAPES = {"w_gate": (LAYERS, D, FF), "w_up": (LAYERS, D, FF), "w_down": (LAYERS, FF, D)}


def bump(key, n, height):
    away = (jnp.arange(n, dtype=jnp.int32) - jax.random.randint(key, (), 0, n, jnp.int32)) % n
    return jnp.where(away < n // 8, height, 1.0)


def together(key, own, strength):
    shared = jax.random.normal(key, own.shape[1:], jnp.float32)
    return (own + strength * shared) * lax.rsqrt(1 + strength * strength)


def setup_inputs(seed: int = 0, part: int = 0) -> dict:
    kx, kdy, ka, kb, kz, kf, kh, kl, *keys = jax.random.split(jax.random.key(seed), 8 + 3 * len(NAMES))
    kx, kdy, ka, kb = (jax.random.fold_in(k, part) for k in (kx, kdy, ka, kb))
    kw, km, kv = (keys[i::3] for i in range(3))
    shape = (SEQUENCES, TOKENS, D)
    much_x, much_dy = jax.random.uniform(kz, (2,), jnp.float32, 0.0, 1.0)
    loud = 2.0 ** jax.random.uniform(jax.random.fold_in(kz, 1), (), jnp.float32, -1.0, 2.0)
    layers = 2.0 ** jax.random.uniform(kl, (LAYERS, 1, 1), jnp.float32, -1.0, 1.0)
    x = together(ka, jax.random.normal(kx, shape, jnp.float32), much_x) * bump(kf, D, 4.0)
    dy = together(kb, jax.random.normal(kdy, shape, jnp.float32), much_dy)
    drawn = {"x": x.astype(jnp.bfloat16), "dy": (loud * dy * (SEQUENCES * TOKENS) ** -0.5).astype(jnp.bfloat16)}
    for key, name in zip(kw, NAMES, strict=True):
        w = jax.random.normal(key, SHAPES[name], jnp.float32) * SHAPES[name][1] ** -0.5
        drawn[name] = (w * {"w_gate": 1.0, "w_up": bump(kh, FF, 4.0), "w_down": layers}[name]).astype(jnp.bfloat16)
    for key, name in zip(km, NAMES, strict=True):
        drawn[f"m_{name}"] = 0.1 * jax.random.normal(key, SHAPES[name], jnp.float32)
    for key, name in zip(kv, NAMES, strict=True):
        drawn[f"v_{name}"] = jax.random.uniform(key, SHAPES[name], jnp.float32, 0.005, 0.015)
    return drawn


def matmul(a, w):
    return jnp.dot(a, w, preferred_element_type=jnp.float32).astype(jnp.bfloat16)


def normed(h):
    wide = h.astype(jnp.float32)
    scale = lax.rsqrt(jnp.mean(wide**2, -1, keepdims=True) + 1e-6)
    return (wide * scale).astype(jnp.bfloat16)


def layer(h, w):
    a = normed(h)
    gate = jnp.dot(a, w["w_gate"], preferred_element_type=jnp.float32)
    up = jnp.dot(a, w["w_up"], preferred_element_type=jnp.float32)
    return h + matmul((jax.nn.silu(gate) * up).astype(jnp.bfloat16), w["w_down"])


def adamw(w, m, v, g):
    m = 0.9 * m + 0.1 * g
    v = 0.95 * v + 0.05 * g * g
    step = m * lax.rsqrt(v + 1e-8) + 0.1 * w
    return (w - 0.02 * step).astype(jnp.bfloat16), m, v


def stack(weights, h):
    return lax.scan(lambda h, w: (layer(h, w), None), h, weights)[0]


def reference(x, dy, w_gate, w_up, w_down, m_w_gate, m_w_up, m_w_down, v_w_gate, v_w_up, v_w_down):
    weights = dict(zip(NAMES, (w_gate, w_up, w_down), strict=True))

    def take(so_far, sequence):
        h, by_y = sequence
        _, back = jax.vjp(lambda w: stack(w, h), weights)
        return jax.tree.map(lambda total, term: total + term.astype(jnp.float32), so_far, back(by_y)[0]), None

    none_yet = {name: jnp.zeros(w.shape, jnp.float32) for name, w in weights.items()}
    by_weights, _ = lax.scan(take, none_yet, (x, dy))
    gradients = [by_weights[name].astype(jnp.bfloat16).astype(jnp.float32) for name in NAMES]
    new = [
        adamw(w.astype(jnp.float32), m, v, g)
        for w, m, v, g in zip((w_gate, w_up, w_down), (m_w_gate, m_w_up, m_w_down), (v_w_gate, v_w_up, v_w_down), gradients, strict=True)
    ]
    return tuple(one[which] for which in range(3) for one in new)
```

```python
import jax
import jax.numpy as jnp
from jax import lax
from jax.experimental import pallas as pl
from jax.experimental.pallas import tpu as pltpu
from jax.sharding import PartitionSpec as P

NAMES = ("w_gate", "w_up", "w_down")
F32, BF16 = jnp.float32, jnp.bfloat16
T, D, FF, L = 2048, 640, 2048, 2
C = 256
PER = FF // C
N = L * PER
NS = 6
R = 3 * D
Q = R // 4
STEPS = N + 5
MESH = pl.DeviceIdType.MESH
NT = (((1,), (1,)), ((), ()))


def normed(h):
    wide = h.astype(F32)
    scale = lax.rsqrt(jnp.mean(wide**2, -1, keepdims=True) + 1e-6)
    return (wide * scale).astype(BF16)


def dot(a, b):
    return jnp.dot(a, b, preferred_element_type=F32)


def add(*terms):
    total = terms[0].astype(F32)
    for term in terms[1:]:
        total = total + term.astype(F32)
    return total.astype(BF16)


def backward_kernel(
    a1, a1t, dy, dyt, h1, a0, a0t, wg, wu, wd, out_g, out_u, out_d,
    A, AT, DY, DYT, H, DA, ACT, DG, DU, WG, WU, WD, OT,
    G, DD, YR, ZR1, XR, ZR2, MR, YX, ST1, ST2, ST3,
    ld, ws, outs, sent, got,
):
    rep, dp = lax.axis_index("rep"), lax.axis_index("dp")
    core, z, y = lax.rem(dp, 2), lax.rem(dp // 2, 4), dp // 8
    at = lambda y, z, core: (rep, (y * 4 + z) * 2 + core)
    zo = z + 1 - 2 * lax.rem(z, 2)
    partner, across, end, mid = at(y, z, 1 - core), at(1 - y, z, core), at(y, zo, core), at(y, 3 - z, core)
    inner = (z == 1) | (z == 2)
    outer = (z == 0) | (z == 3)
    mi = lax.rem(z + 1, 2)
    mine_y, their_y = pl.multiple_of(y * Q, 16), pl.multiple_of((1 - y) * Q, 16)
    mine_m, their_m = pl.multiple_of(2 * Q + mi * Q, 16), pl.multiple_of(2 * Q + (1 - mi) * Q, 16)
    mine_y, their_y, mine_m, their_m = (pl.ds(start, Q) for start in (mine_y, their_y, mine_m, their_m))
    low = pl.ds(2 * Q, 2 * Q)

    def loads():
        return [pltpu.make_async_copy(s, d, ld.at[i]) for i, (s, d) in enumerate(((a1, A), (dy, DY), (a1t, AT), (dyt, DYT), (h1, H)))]

    def weights(i):
        layer, j, s = L - 1 - i // PER, lax.rem(i, PER), lax.rem(i, 2)
        cols = pl.ds(pl.multiple_of(j * C, C), C)
        return [
            pltpu.make_async_copy(wg.at[layer, :, cols], WG.at[s], ws.at[s, 0]),
            pltpu.make_async_copy(wu.at[layer, :, cols], WU.at[s], ws.at[s, 1]),
            pltpu.make_async_copy(wd.at[layer, cols, :], WD.at[s], ws.at[s, 2]),
        ]

    for copy in loads() + weights(0):
        copy.start()

    barrier = pltpu.get_barrier_semaphore()
    for device in (partner, across, end):
        pl.semaphore_signal(barrier, inc=1, device_id=device, device_id_type=MESH)

    @pl.when(inner)
    def _():
        pl.semaphore_signal(barrier, inc=1, device_id=mid, device_id_type=MESH)

    pl.semaphore_wait(barrier, 3 + inner.astype(jnp.int32))
    DA[...] = jnp.zeros_like(DA)
    for copy in loads():
        copy.wait()

    def copies(q):
        def remote(n, src, dst, device):
            return pltpu.make_async_remote_copy(
                src_ref=src, dst_ref=dst, send_sem=sent.at[n, q], recv_sem=got.at[n, q], device_id=device, device_id_type=MESH
            )

        own = G.at[q, core]
        made = dict(
            d1=lambda: remote(0, G.at[q, 1 - core], DD.at[q], partner),
            y1=lambda: remote(1, ST1.at[q], YR.at[q], across),
            z2=lambda: remote(2, ST2.at[q], ZR2.at[q], end),
            z1=lambda: remote(3, ST3.at[q], ZR1.at[q], end),
            m2=lambda: remote(4, ST2.at[q, pl.ds(0, Q)], MR.at[q], mid),
            x1=lambda: remote(5, ST3.at[q], XR.at[q], mid),
            y2=lambda: remote(6, ST2.at[q, pl.ds(Q, Q)], YX.at[q], across),
            f1=lambda: remote(7, own.at[mine_y], own.at[mine_y], end),
            f2=lambda: remote(8, own.at[mine_y], own.at[mine_y], across),
            g1=lambda: remote(9, own.at[mine_m], own.at[mine_m], mid),
            g2=lambda: remote(10, own.at[mine_m], own.at[mine_m], end),
            g3=lambda: remote(11, own.at[their_m], own.at[their_m], end),
            d2=lambda: remote(12, own, own, partner),
        )
        return lambda name: made[name]()

    def out_copies(c):
        layer, j, q, s = L - 1 - c // PER, lax.rem(c, PER), lax.rem(c, NS), lax.rem(c, 2)
        made = []
        for half in range(2):
            cols = pl.ds(pl.multiple_of(j * C + half * 128, 128), 128)
            made.append(pltpu.make_async_copy(G.at[q, half, pl.ds(0, D)], out_g.at[layer, :, cols], outs.at[s, half]))
            made.append(pltpu.make_async_copy(G.at[q, half, pl.ds(D, D)], out_u.at[layer, :, cols], outs.at[s, 2 + half]))
        rows = pl.ds(pl.multiple_of(j * C, C), C)
        made.append(pltpu.make_async_copy(OT.at[s], out_d.at[layer, rows, :], outs.at[s, 4]))
        return made

    def stage_d1(q, c):
        c("d1").start()

    def stage_first(q, c):
        c("d1").wait()
        ST1[q] = add(G[q, core, their_y], DD[q, their_y])
        c("y1").start()

        @pl.when(outer)
        def _():
            ST2[q] = add(G[q, core, low], DD[q, low])
            c("z2").start()

    def stage_z1(q, c):
        @pl.when(outer)
        def _():
            c("y1").wait_recv()
            ST3[q] = add(G[q, core, mine_y], DD[q, mine_y], YR[q])
            c("z1").start()

    def stage_m2(q, c):
        @pl.when(inner)
        def _():
            c("z2").wait_recv()
            ST2[q, pl.ds(0, Q)] = add(G[q, core, their_m], DD[q, their_m], ZR2[q, pl.ds(pl.multiple_of((1 - mi) * Q, 16), Q)])
            c("m2").start()

    def stage_x1(q, c):
        @pl.when(inner)
        def _():
            c("y1").wait_recv()
            c("z1").wait_recv()
            ST3[q] = add(G[q, core, mine_y], DD[q, mine_y], YR[q], ZR1[q])
            c("x1").start()

    def stage_y2(q, c):
        @pl.when(inner)
        def _():
            c("m2").wait_recv()
            ST2[q, pl.ds(Q, Q)] = add(G[q, core, mine_m], DD[q, mine_m], ZR2[q, pl.ds(pl.multiple_of(mi * Q, 16), Q)], MR[q])
            c("y2").start()

    def stage_f(q, c):
        @pl.when(inner)
        def _():
            c("x1").wait()
            G[q, core, mine_y] = add(ST3[q], XR[q])
            c("f1").start()
            c("f2").start()

    def stage_g(q, c):
        @pl.when(inner)
        def _():
            c("y2").wait()
            G[q, core, mine_m] = add(ST2[q, pl.ds(Q, Q)], YX[q])
            c("g1").start()
            c("g2").start()

    def stage_f2(q, c):
        @pl.when(outer)
        def _():
            c("f1").wait_recv()
            c("f2").start()

    def stage_g3(q, c):
        @pl.when(inner)
        def _():
            c("g1").wait_recv()
            c("g3").start()

    def stage_d2(q, c):
        c("f2").wait_recv()

        @pl.when(outer)
        def _():
            c("g2").wait_recv()
            c("g3").wait_recv()

        c("d2").start()

    def stage_end(q, c):
        c("d2").wait()
        for name in ("y1", "f2"):
            c(name).wait_send()

        @pl.when(outer)
        def _():
            for name in ("z2", "z1"):
                c(name).wait_send()

        @pl.when(inner)
        def _():
            for name in ("m2", "f1", "g1", "g2", "g3"):
                c(name).wait_send()

    STAGES = {
        0: stage_d1, 1: stage_first, 4: stage_z1, 5: stage_m2, 7: stage_x1, 8: stage_y2,
        10: stage_f, 11: stage_g, 13: stage_f2, 14: stage_g3, 17: stage_d2,
    }
    END = 18

    def tick(i, k):
        for when, stage in sorted(STAGES.items(), reverse=True):
            if when % 4 != k:
                continue
            c = i - 1 - when // 4

            @pl.when((c >= 0) & (c < N))
            def _(c=c, stage=stage):
                q = lax.rem(c, NS)
                stage(q, copies(q))

        if END % 4 == k:
            c = i - 1 - END // 4

            @pl.when((c >= 0) & (c < N))
            def _():
                q, s = lax.rem(c, NS), lax.rem(c, 2)

                @pl.when(c >= 1)
                def _():
                    for copy in out_copies(c - 1):
                        copy.wait()

                stage_end(q, copies(q))
                for half in range(2):
                    OT[s, pl.ds(half * 128, 128), :] = G[q, half, pl.ds(2 * D, D)].astype(F32).T.astype(BF16)
                for copy in out_copies(c):
                    copy.start()

    def tokens(s, first):
        def block(b, _):
            rows = pl.ds(pl.multiple_of(first + b * 512, 512), 512)
            a = A[rows]
            gate, up = dot(a, WG[s]), dot(a, WU[s])
            dact = lax.dot_general(DY[rows], WD[s], NT, preferred_element_type=F32).astype(BF16).astype(F32)
            sig = 1.0 / (1.0 + jnp.exp(-gate))
            silu = gate * sig
            ACT[rows] = (silu * up).astype(BF16)
            DU[rows] = (dact * silu).astype(BF16)
            DG[rows] = (dact * up * (sig + silu * (1.0 - sig))).astype(BF16)
            return _

        lax.fori_loop(0, 2, block, None)

    def gradient(q, which, left, right):
        def block(b, _):
            rows = pl.multiple_of(b * 128, 128)
            g = dot(left[pl.ds(rows, 128)], right[...]).astype(BF16)
            to = pl.ds(pl.multiple_of(which * D + rows, 128), 128)
            G[q, 0, to] = g[:, :128]
            G[q, 1, to] = g[:, 128:]
            return _

        lax.fori_loop(0, D // 128, block, None)

    def switch():
        copies = [pltpu.make_async_copy(a0, A, ld.at[0]), pltpu.make_async_copy(a0t, AT, ld.at[2])]
        for copy in copies:
            copy.start()

        def block(b, _):
            rows = pl.ds(pl.multiple_of(b * 256, 256), 256)
            h = H[rows].astype(F32)
            da = DA[rows].astype(BF16).astype(F32)
            scale = lax.rsqrt(jnp.mean(h * h, -1, keepdims=True) + 1e-6)
            along = jnp.sum(da * h, -1, keepdims=True) * (1.0 / D)
            dh = (scale * (da - h * (scale * scale * along))).astype(BF16)
            new = DY[rows].astype(F32) + dh.astype(F32)
            DY[rows] = new.astype(BF16)
            DYT[:, rows] = new.T.astype(BF16)
            return _

        lax.fori_loop(0, T // 256, block, None)
        for copy in copies:
            copy.wait()

    def step(i, _):
        busy = i < N
        s, q = lax.rem(i, 2), lax.rem(i, NS)

        tick(i, 0)

        @pl.when(i == PER)
        def _():
            switch()

        @pl.when(busy)
        def _():
            for copy in weights(i):
                copy.wait()

            @pl.when(i + 1 < N)
            def _():
                for copy in weights(i + 1):
                    copy.start()

            tokens(s, 0)

        tick(i, 1)

        @pl.when(busy)
        def _():
            tokens(s, 1024)

        tick(i, 2)

        @pl.when(busy)
        def _():
            gradient(q, 0, AT, DG)
            gradient(q, 1, AT, DU)

        tick(i, 3)

        @pl.when(busy)
        def _():
            gradient(q, 2, DYT, ACT)

        @pl.when(i < PER)
        def _():
            def block(b, _):
                rows = pl.ds(pl.multiple_of(b * 512, 512), 512)
                DA[rows] += lax.dot_general(DG[rows], WG[s], NT, preferred_element_type=F32) + lax.dot_general(
                    DU[rows], WU[s], NT, preferred_element_type=F32
                )
                return _

            lax.fori_loop(0, T // 512, block, None)

        return _

    lax.fori_loop(0, STEPS, step, None)
    for copy in out_copies(N - 1):
        copy.wait()


def backward(a1, a1t, dy, dyt, h1, a0, a0t, wg, wu, wd):
    vm = pltpu.VMEM
    return pl.pallas_call(
        backward_kernel,
        out_shape=[jax.ShapeDtypeStruct(w.shape, BF16) for w in (wg, wu, wd)],
        in_specs=[pl.BlockSpec(memory_space=pl.ANY)] * 10,
        out_specs=[pl.BlockSpec(memory_space=pl.ANY)] * 3,
        scratch_shapes=[
            vm((T, D), BF16), vm((D, T), BF16), vm((T, D), BF16), vm((D, T), BF16), vm((T, D), BF16), vm((T, D), F32),
            vm((T, C), BF16), vm((T, C), BF16), vm((T, C), BF16),
            vm((2, D, C), BF16), vm((2, D, C), BF16), vm((2, C, D), BF16), vm((2, C, D), BF16),
            vm((NS, 2, R, 128), BF16), vm((NS, R, 128), BF16), vm((NS, Q, 128), BF16), vm((NS, Q, 128), BF16), vm((NS, Q, 128), BF16),
            vm((NS, 2 * Q, 128), BF16), vm((NS, Q, 128), BF16), vm((NS, Q, 128), BF16),
            vm((NS, Q, 128), BF16), vm((NS, 2 * Q, 128), BF16), vm((NS, Q, 128), BF16),
            pltpu.SemaphoreType.DMA((5,)), pltpu.SemaphoreType.DMA((2, 3)), pltpu.SemaphoreType.DMA((2, 5)),
            pltpu.SemaphoreType.DMA((13, NS)), pltpu.SemaphoreType.DMA((13, NS)),
        ],
        compiler_params=pltpu.CompilerParams(collective_id=0, has_side_effects=True, vmem_limit_bytes=60 * 2**20),
    )(a1, a1t, dy, dyt, h1, a0, a0t, wg, wu, wd)


def adamw(w, m, v, g):
    m = 0.9 * m + 0.1 * g
    v = 0.95 * v + 0.05 * g * g
    step = m * lax.rsqrt(v + 1e-8) + 0.1 * w
    return (w - 0.02 * step).astype(BF16), m, v


def solution(mesh):
    def step(x, dy, *arrays):
        weights, m, v = (arrays[i : i + 3] for i in (0, 3, 6))
        wg, wu, wd = weights
        x, dy = x[0], dy[0]
        a0 = normed(x)
        act = (jax.nn.silu(dot(a0, wg[0])) * dot(a0, wu[0])).astype(BF16)
        h1 = x + dot(act, wd[0]).astype(BF16)
        a1 = normed(h1)
        gradients = backward(a1, a1.T, dy, dy.T, h1, a0, a0.T, wg, wu, wd)
        new = [adamw(w.astype(F32), m, v, g.astype(F32)) for w, m, v, g in zip(weights, m, v, gradients, strict=True)]
        return tuple(one[which] for which in range(3) for one in new)

    return jax.shard_map(
        step,
        mesh=mesh,
        in_specs=(P(("rep", "dp"), None, None),) * 2 + (P(None, None, None),) * 9,
        out_specs=(P("rep", None, None),) * 9,
        check_vma=False,
    )
```

```python
import jax
import jax.numpy as jnp
from jax import lax
from jax.experimental import pallas as pl
from jax.experimental.pallas import tpu as pltpu
from jax.sharding import PartitionSpec as P

NAMES = ("w_gate", "w_up", "w_down")
F32, BF16 = jnp.float32, jnp.bfloat16
T, D, FF, L = 2048, 640, 2048, 2
C = 256
PER = FF // C
N = L * PER
PIECES = 2 * N
NS = 10
R = 3 * D // 2
Q = R // 4
MESH = pl.DeviceIdType.MESH
NT = (((1,), (1,)), ((), ()))


def normed(h):
    wide = h.astype(F32)
    scale = lax.rsqrt(jnp.mean(wide**2, -1, keepdims=True) + 1e-6)
    return (wide * scale).astype(BF16)


def dot(a, b):
    return jnp.dot(a, b, preferred_element_type=F32)


def dot_nt(a, b):
    return lax.dot_general(a, b, NT, preferred_element_type=F32)


def sigmoid(a):
    return 0.5 * jnp.tanh(0.5 * a) + 0.5


def add(*terms):
    total = terms[0].astype(F32)
    for term in terms[1:]:
        total = total + term.astype(F32)
    return total.astype(BF16)


def step_kernel(
    x, dy, wg, wu, wd, out_g, out_u, out_d,
    A, AT, DY, DYT, H, DA, ACT, DGU, ACTF, WF, WU, WFD, WGU, WD, OT,
    G, DD, YR, ZR1, XR, ZR2, MR, YX, ST1, ST2, ST3,
    ld, ws, outs, sent, got,
):
    rep, dp = lax.axis_index("rep"), lax.axis_index("dp")
    core, z, y = lax.rem(dp, 2), lax.rem(dp // 2, 4), dp // 8
    at = lambda y, z, core: (rep, (y * 4 + z) * 2 + core)
    zo = z + 1 - 2 * lax.rem(z, 2)
    partner, across, end, mid = at(y, z, 1 - core), at(1 - y, z, core), at(y, zo, core), at(y, 3 - z, core)
    inner = (z == 1) | (z == 2)
    outer = (z == 0) | (z == 3)
    mi = lax.rem(z + 1, 2)
    mine_y, their_y = pl.multiple_of(y * Q, 16), pl.multiple_of((1 - y) * Q, 16)
    mine_m, their_m = pl.multiple_of(2 * Q + mi * Q, 16), pl.multiple_of(2 * Q + (1 - mi) * Q, 16)
    mine_y, their_y, mine_m, their_m = (pl.ds(start, Q) for start in (mine_y, their_y, mine_m, their_m))
    low = pl.ds(2 * Q, 2 * Q)

    def loads():
        pairs = ((x.at[0], H), (wg.at[0], WF), (wu.at[0], WU), (wd.at[0], WFD), (dy.at[0], DY))
        return [pltpu.make_async_copy(s, d, ld.at[i]) for i, (s, d) in enumerate(pairs)]

    def weights(i):
        layer, j, s = L - 1 - i // PER, lax.rem(i, PER), lax.rem(i, 2)
        cols = pl.ds(pl.multiple_of(j * C, C), C)
        return [
            pltpu.make_async_copy(wg.at[layer, :, cols], WGU.at[s, :, pl.ds(0, C)], ws.at[s, 0]),
            pltpu.make_async_copy(wu.at[layer, :, cols], WGU.at[s, :, pl.ds(C, C)], ws.at[s, 1]),
            pltpu.make_async_copy(wd.at[layer, cols, :], WD.at[s], ws.at[s, 2]),
        ]

    for copy in loads() + weights(0):
        copy.start()

    barrier = pltpu.get_barrier_semaphore()
    for device in (partner, across, end):
        pl.semaphore_signal(barrier, inc=1, device_id=device, device_id_type=MESH)

    @pl.when(inner)
    def _():
        pl.semaphore_signal(barrier, inc=1, device_id=mid, device_id_type=MESH)

    DA[...] = jnp.zeros_like(DA)
    for copy in loads():
        copy.wait()

    def forward(b, _):
        rows = pl.ds(pl.multiple_of(b * 512, 512), 512)
        x = H[rows]
        a = normed(x)
        A[0, rows] = a
        AT[0, :, rows] = a.T
        DYT[:, rows] = DY[rows].T
        for k in range(4):
            cols = pl.ds(k * 512, 512)
            gate, up = dot(a, WF[:, cols]), dot(a, WU[:, cols])
            ACTF[:, cols] = (gate * sigmoid(gate) * up).astype(BF16)
        h = add(x, dot(ACTF[...], WFD[...]).astype(BF16))
        H[rows] = h
        a = normed(h)
        A[1, rows] = a
        AT[1, :, rows] = a.T
        return _

    lax.fori_loop(0, T // 512, forward, None)
    pl.semaphore_wait(barrier, 3 + inner.astype(jnp.int32))

    def copies(q):
        def remote(n, src, dst, device):
            return pltpu.make_async_remote_copy(
                src_ref=src, dst_ref=dst, send_sem=sent.at[n, q], recv_sem=got.at[n, q], device_id=device, device_id_type=MESH
            )

        own = G.at[q, core]
        made = dict(
            d1=lambda: remote(0, G.at[q, 1 - core], DD.at[q], partner),
            y1=lambda: remote(1, ST1.at[q], YR.at[q], across),
            z2=lambda: remote(2, ST2.at[q], ZR2.at[q], end),
            z1=lambda: remote(3, ST3.at[q], ZR1.at[q], end),
            m2=lambda: remote(4, ST2.at[q, pl.ds(0, Q)], MR.at[q], mid),
            x1=lambda: remote(5, ST3.at[q], XR.at[q], mid),
            y2=lambda: remote(6, ST2.at[q, pl.ds(Q, Q)], YX.at[q], across),
            f1=lambda: remote(7, own.at[mine_y], own.at[mine_y], end),
            f2=lambda: remote(8, own.at[mine_y], own.at[mine_y], across),
            g1=lambda: remote(9, own.at[mine_m], own.at[mine_m], mid),
            g2=lambda: remote(10, own.at[mine_m], own.at[mine_m], end),
            g3=lambda: remote(11, own.at[their_m], own.at[their_m], end),
            d2=lambda: remote(12, own, own, partner),
        )
        return lambda name: made[name]()

    def out_copies(c, odd):
        layer, j, q, s = L - 1 - c // (2 * PER), lax.rem(c // 2, PER), lax.rem(c, NS), lax.rem(c // 2, 2)
        made = []
        for half in range(2):
            cols = pl.ds(pl.multiple_of(j * C + half * 128, 128), 128)
            if odd:
                made.append(pltpu.make_async_copy(G.at[q, half, pl.ds(0, D // 2)], out_u.at[layer, pl.ds(D // 2, D // 2), cols], outs.at[1, half]))
            else:
                made.append(pltpu.make_async_copy(G.at[q, half, pl.ds(0, D)], out_g.at[layer, :, cols], outs.at[0, half]))
                made.append(pltpu.make_async_copy(G.at[q, half, pl.ds(D, D // 2)], out_u.at[layer, pl.ds(0, D // 2), cols], outs.at[0, 2 + half]))
        if odd:
            rows = pl.ds(pl.multiple_of(j * C, C), C)
            made.append(pltpu.make_async_copy(OT.at[s], out_d.at[layer, rows, :], outs.at[1, 4]))
        return made

    def stage_d1(q, c):
        c("d1").start()

    def stage_first(q, c):
        c("d1").wait()
        ST1[q] = add(G[q, core, their_y], DD[q, their_y])
        c("y1").start()

        @pl.when(outer)
        def _():
            ST2[q] = add(G[q, core, low], DD[q, low])
            c("z2").start()

    def stage_z1(q, c):
        @pl.when(outer)
        def _():
            c("y1").wait_recv()
            ST3[q] = add(G[q, core, mine_y], DD[q, mine_y], YR[q])
            c("z1").start()

    def stage_m2(q, c):
        @pl.when(inner)
        def _():
            c("z2").wait_recv()
            ST2[q, pl.ds(0, Q)] = add(G[q, core, their_m], DD[q, their_m], ZR2[q, pl.ds(pl.multiple_of((1 - mi) * Q, 16), Q)])
            c("m2").start()

    def stage_x1(q, c):
        @pl.when(inner)
        def _():
            c("y1").wait_recv()
            c("z1").wait_recv()
            ST3[q] = add(G[q, core, mine_y], DD[q, mine_y], YR[q], ZR1[q])
            c("x1").start()

    def stage_y2(q, c):
        @pl.when(inner)
        def _():
            c("m2").wait_recv()
            ST2[q, pl.ds(Q, Q)] = add(G[q, core, mine_m], DD[q, mine_m], ZR2[q, pl.ds(pl.multiple_of(mi * Q, 16), Q)], MR[q])
            c("y2").start()

    def stage_f(q, c):
        @pl.when(inner)
        def _():
            c("x1").wait()
            G[q, core, mine_y] = add(ST3[q], XR[q])
            c("f1").start()
            c("f2").start()

    def stage_g(q, c):
        @pl.when(inner)
        def _():
            c("y2").wait()
            G[q, core, mine_m] = add(ST2[q, pl.ds(Q, Q)], YX[q])
            c("g1").start()
            c("g2").start()

    def stage_f2(q, c):
        @pl.when(outer)
        def _():
            c("f1").wait_recv()
            c("f2").start()

    def stage_g3(q, c):
        @pl.when(inner)
        def _():
            c("g1").wait_recv()
            c("g3").start()

    def stage_d2(q, c):
        c("f2").wait_recv()

        @pl.when(outer)
        def _():
            c("g2").wait_recv()
            c("g3").wait_recv()

        c("d2").start()

    def stage_end(q, c):
        c("d2").wait()
        for name in ("y1", "f2"):
            c(name).wait_send()

        @pl.when(outer)
        def _():
            for name in ("z2", "z1"):
                c(name).wait_send()

        @pl.when(inner)
        def _():
            for name in ("m2", "f1", "g1", "g2", "g3"):
                c(name).wait_send()

    STAGES = {
        0: stage_d1, 1: stage_first, 3: stage_z1, 4: stage_m2, 5: stage_x1, 6: stage_y2,
        7: stage_f, 8: stage_g, 9: stage_f2, 10: stage_g3, 12: stage_d2,
    }
    END = 13

    def finish(c, odd):
        q, s = lax.rem(c, NS), lax.rem(c // 2, 2)

        @pl.when(c >= 1)
        def _():
            for copy in out_copies(c - 1, not odd):
                copy.wait()

        stage_end(q, copies(q))
        if odd:
            for half in range(2):
                OT[s, pl.ds(half * 128, 128), :] = G[q, half, pl.ds(D // 2, D)].T
        for copy in out_copies(c, odd):
            copy.start()

    def tick(u, k):
        for when, stage in sorted(STAGES.items(), reverse=True):
            if when % 2 != k:
                continue
            c = u - 2 - when // 2

            @pl.when((c >= 0) & (c < PIECES))
            def _(c=c, stage=stage):
                q = lax.rem(c, NS)
                stage(q, copies(q))

        if END % 2 == k:
            c = u - 2 - END // 2
            for odd in (False, True):

                @pl.when((c >= 0) & (c < PIECES) & (lax.rem(c + 2, 2) == int(odd)))
                def _(odd=odd):
                    finish(c, odd)

    def tokens(s, layer, first):
        for b in range(2):
            rows = pl.ds(first + b * 512, 512)
            gu = dot(A[layer, rows], WGU[s])
            gate, up = gu[:, :C], gu[:, C:]
            dact = dot_nt(DY[rows], WD[s]).astype(BF16).astype(F32)
            sig = sigmoid(gate)
            silu = gate * sig
            ACT[rows] = (silu * up).astype(BF16)
            DGU[rows, pl.ds(0, C)] = (dact * up * (sig + silu * (1.0 - sig))).astype(BF16)
            DGU[rows, pl.ds(C, C)] = (dact * silu).astype(BF16)

    def switch():
        def block(b, _):
            rows = pl.ds(pl.multiple_of(b * 256, 256), 256)
            h = H[rows].astype(F32)
            da = DA[rows].astype(BF16).astype(F32)
            scale = lax.rsqrt(jnp.mean(h * h, -1, keepdims=True) + 1e-6)
            along = jnp.sum(da * h, -1, keepdims=True) * (1.0 / D)
            dh = (scale * (da - h * (scale * scale * along))).astype(BF16)
            new = add(DY[rows], dh)
            DY[rows] = new
            DYT[:, rows] = new.T
            return _

        lax.fori_loop(0, T // 256, block, None)

    def step(u, _):
        i = u // 2
        busy = i < N
        even, odd = busy & (lax.rem(u, 2) == 0), busy & (lax.rem(u, 2) == 1)
        s, layer = lax.rem(i, 2), jnp.maximum(L - 1 - i // PER, 0)
        first, second = lax.rem(2 * i, NS), lax.rem(2 * i + 1, NS)

        tick(u, 0)

        @pl.when(u == 2 * PER)
        def _():
            switch()

        @pl.when(even)
        def _():
            for copy in weights(i):
                copy.wait()

            @pl.when(i + 1 < N)
            def _():
                for copy in weights(i + 1):
                    copy.start()

            tokens(s, layer, 0)

        @pl.when(odd)
        def _():
            g = dot(AT[layer], DGU[...]).astype(BF16)
            for half in range(2):
                cols = slice(half * 128, half * 128 + 128)
                G[first, half, pl.ds(0, D)] = g[:, cols]
                cols = slice(C + half * 128, C + half * 128 + 128)
                G[first, half, pl.ds(D, D // 2)] = g[: D // 2, cols]
                G[second, half, pl.ds(0, D // 2)] = g[D // 2 :, cols]

        tick(u, 1)

        @pl.when(even)
        def _():
            tokens(s, layer, T // 2)

        @pl.when(odd)
        def _():
            g = dot(DYT[...], ACT[...]).astype(BF16)
            for half in range(2):
                G[second, half, pl.ds(D // 2, D)] = g[:, half * 128 : half * 128 + 128]

        @pl.when(odd & (i < PER))
        def _():
            for b in range(2):
                rows = pl.ds(b * 1024, 1024)
                DA[rows] += dot_nt(DGU[rows], WGU[s])

        return _

    lax.fori_loop(0, PIECES + 2 + END // 2 + 1, step, None)
    for copy in out_copies(PIECES - 1, True):
        copy.wait()


def gradients_of(x, dy, wg, wu, wd):
    vm, dma = pltpu.VMEM, pltpu.SemaphoreType.DMA
    return pl.pallas_call(
        step_kernel,
        out_shape=[jax.ShapeDtypeStruct(w.shape, BF16) for w in (wg, wu, wd)],
        in_specs=[pl.BlockSpec(memory_space=pl.ANY)] * 5,
        out_specs=[pl.BlockSpec(memory_space=pl.ANY)] * 3,
        scratch_shapes=[
            vm((L, T, D), BF16), vm((L, D, T), BF16), vm((T, D), BF16), vm((D, T), BF16), vm((T, D), BF16), vm((T, D), F32),
            vm((T, C), BF16), vm((T, 2 * C), BF16), vm((512, FF), BF16),
            vm((D, FF), BF16), vm((D, FF), BF16), vm((FF, D), BF16),
            vm((2, D, 2 * C), BF16), vm((2, C, D), BF16), vm((2, C, D), BF16),
            vm((NS, 2, R, 128), BF16), vm((NS, R, 128), BF16), vm((NS, Q, 128), BF16), vm((NS, Q, 128), BF16), vm((NS, Q, 128), BF16),
            vm((NS, 2 * Q, 128), BF16), vm((NS, Q, 128), BF16), vm((NS, Q, 128), BF16),
            vm((NS, Q, 128), BF16), vm((NS, 2 * Q, 128), BF16), vm((NS, Q, 128), BF16),
            dma((5,)), dma((2, 3)), dma((2, 5)), dma((13, NS)), dma((13, NS)),
        ],
        compiler_params=pltpu.CompilerParams(collective_id=0, has_side_effects=True, vmem_limit_bytes=67043328),
    )(x, dy, wg, wu, wd)


def adamw(w, m, v, g):
    m = 0.9 * m + 0.1 * g
    v = 0.95 * v + 0.05 * g * g
    step = m * lax.rsqrt(v + 1e-8) + 0.1 * w
    return (w - 0.02 * step).astype(BF16), m, v


def solution(mesh):
    def step(x, dy, *arrays):
        weights, m, v = (arrays[i : i + 3] for i in (0, 3, 6))
        gradients = gradients_of(x, dy, *weights)
        new = [adamw(w.astype(F32), m, v, g.astype(F32)) for w, m, v, g in zip(weights, m, v, gradients, strict=True)]
        return tuple(one[which] for which in range(3) for one in new)

    return jax.shard_map(
        step,
        mesh=mesh,
        in_specs=(P(("rep", "dp"), None, None),) * 2 + (P(None, None, None),) * 9,
        out_specs=(P("rep", None, None),) * 9,
        check_vma=False,
    )
```

```python
import jax
import jax.numpy as jnp
from jax import lax
from jax.experimental import pallas as pl
from jax.experimental.pallas import tpu as pltpu
from jax.sharding import PartitionSpec as P

NAMES = ("w_gate", "w_up", "w_down")
F32, BF16 = jnp.float32, jnp.bfloat16
T, D, FF, L = 2048, 640, 2048, 2
C = 256
PER = FF // C
N = L * PER
PIECES = 2 * N
NS = 12
R = 3 * D // 2
Q = R // 4
MESH = pl.DeviceIdType.MESH
NT = (((1,), (1,)), ((), ()))


def normed(h):
    wide = h.astype(F32)
    scale = lax.rsqrt(jnp.mean(wide**2, -1, keepdims=True) + 1e-6)
    return (wide * scale).astype(BF16)


def dot(a, b):
    return jnp.dot(a, b, preferred_element_type=F32)


def dot_nt(a, b):
    return lax.dot_general(a, b, NT, preferred_element_type=F32)


def sigmoid(a):
    return 0.5 * jnp.tanh(0.5 * a) + 0.5


def add(*terms):
    total = terms[0].astype(F32)
    for term in terms[1:]:
        total = total + term.astype(F32)
    return total.astype(BF16)


def step_kernel(
    x, dy, wg, wu, wd, out_g, out_u, out_d,
    A, AT, DY, DYT, H, DA, ACT, DGU, ACTF, WF, WU, WFD, WGU, WD, OT,
    G, DD, YR, ZR1, XR, ZR2, MR, YX, ST1, ST2, ST3,
    ld, ws, outs, sent, got,
):
    rep, dp = lax.axis_index("rep"), lax.axis_index("dp")
    core, z, y = lax.rem(dp, 2), lax.rem(dp // 2, 4), dp // 8
    at = lambda y, z, core: (rep, (y * 4 + z) * 2 + core)
    zo = z + 1 - 2 * lax.rem(z, 2)
    partner, across, end, mid = at(y, z, 1 - core), at(1 - y, z, core), at(y, zo, core), at(y, 3 - z, core)
    inner = (z == 1) | (z == 2)
    outer = (z == 0) | (z == 3)
    mi = lax.rem(z + 1, 2)
    mine_y, their_y = pl.multiple_of(y * Q, 16), pl.multiple_of((1 - y) * Q, 16)
    mine_m, their_m = pl.multiple_of(2 * Q + mi * Q, 16), pl.multiple_of(2 * Q + (1 - mi) * Q, 16)
    mine_y, their_y, mine_m, their_m = (pl.ds(start, Q) for start in (mine_y, their_y, mine_m, their_m))
    low = pl.ds(2 * Q, 2 * Q)

    def loads():
        start, rest = pl.ds(0, 512), pl.ds(512, T - 512)
        pairs = [(x.at[0, start], H.at[start])]
        for k in range(4):
            cols = pl.ds(k * 512, 512)
            pairs += [(wg.at[0, :, cols], WF.at[:, cols]), (wu.at[0, :, cols], WU.at[:, cols])]
        pairs += [(wd.at[0], WFD), (dy.at[0], DY), (x.at[0, rest], H.at[rest])]
        return [pltpu.make_async_copy(s, d, ld.at[i]) for i, (s, d) in enumerate(pairs)]

    def weights(i):
        layer, j, s = L - 1 - i // PER, lax.rem(i, PER), lax.rem(i, 2)
        cols = pl.ds(pl.multiple_of(j * C, C), C)
        return [
            pltpu.make_async_copy(wg.at[layer, :, cols], WGU.at[s, :, pl.ds(0, C)], ws.at[s, 0]),
            pltpu.make_async_copy(wu.at[layer, :, cols], WGU.at[s, :, pl.ds(C, C)], ws.at[s, 1]),
            pltpu.make_async_copy(wd.at[layer, cols, :], WD.at[s], ws.at[s, 2]),
        ]

    arriving = loads()
    for copy in arriving + weights(0):
        copy.start()

    barrier = pltpu.get_barrier_semaphore()
    for device in (partner, across, end):
        pl.semaphore_signal(barrier, inc=1, device_id=device, device_id_type=MESH)

    @pl.when(inner)
    def _():
        pl.semaphore_signal(barrier, inc=1, device_id=mid, device_id_type=MESH)

    def forward(rows, wait):
        wait(0, 1)
        x = H[rows]
        a = normed(x)
        A[0, rows] = a
        AT[0, :, rows] = a.T
        for k in range(4):
            wait(2 * k + 1, 2 * k + 3)
            cols = pl.ds(k * 512, 512)
            gate, up = dot(a, WF[:, cols]), dot(a, WU[:, cols])
            ACTF[:, cols] = (gate * sigmoid(gate) * up).astype(BF16)
        wait(9, 11)
        DYT[:, rows] = DY[rows].T
        DA[rows] = jnp.zeros((512, D), F32)
        h = add(x, dot(ACTF[...], WFD[...]).astype(BF16))
        H[rows] = h
        a = normed(h)
        A[1, rows] = a
        AT[1, :, rows] = a.T

    def now(first, last):
        for copy in arriving[first:last]:
            copy.wait()

    def later(b, _):
        forward(pl.ds(pl.multiple_of(b * 512, 512), 512), lambda first, last: None)
        return _

    forward(pl.ds(0, 512), now)
    now(11, 12)
    lax.fori_loop(1, T // 512, later, None)
    pl.semaphore_wait(barrier, 3 + inner.astype(jnp.int32))

    def copies(q):
        def remote(n, src, dst, device):
            return pltpu.make_async_remote_copy(
                src_ref=src, dst_ref=dst, send_sem=sent.at[n, q], recv_sem=got.at[n, q], device_id=device, device_id_type=MESH
            )

        own = G.at[q, core]
        made = dict(
            d1=lambda: remote(0, G.at[q, 1 - core], DD.at[q], partner),
            y1=lambda: remote(1, ST1.at[q], YR.at[q], across),
            z2=lambda: remote(2, ST2.at[q], ZR2.at[q], end),
            z1=lambda: remote(3, ST3.at[q], ZR1.at[q], end),
            m2=lambda: remote(4, ST2.at[q, pl.ds(0, Q)], MR.at[q], mid),
            x1=lambda: remote(5, ST3.at[q], XR.at[q], mid),
            y2=lambda: remote(6, ST2.at[q, pl.ds(Q, Q)], YX.at[q], across),
            f1=lambda: remote(7, own.at[mine_y], own.at[mine_y], end),
            f2=lambda: remote(8, own.at[mine_y], own.at[mine_y], across),
            g1=lambda: remote(9, own.at[mine_m], own.at[mine_m], mid),
            g2=lambda: remote(10, own.at[mine_m], own.at[mine_m], end),
            g3=lambda: remote(11, own.at[their_m], own.at[their_m], end),
            d2=lambda: remote(12, own, own, partner),
        )
        return lambda name: made[name]()

    def out_copies(c, odd):
        layer, j, q, s = L - 1 - c // (2 * PER), lax.rem(c // 2, PER), lax.rem(c, NS), lax.rem(c // 2, 2)
        made = []
        for half in range(2):
            cols = pl.ds(pl.multiple_of(j * C + half * 128, 128), 128)
            if odd:
                made.append(pltpu.make_async_copy(G.at[q, half, pl.ds(0, D // 2)], out_u.at[layer, pl.ds(D // 2, D // 2), cols], outs.at[1, half]))
            else:
                made.append(pltpu.make_async_copy(G.at[q, half, pl.ds(0, D)], out_g.at[layer, :, cols], outs.at[0, half]))
                made.append(pltpu.make_async_copy(G.at[q, half, pl.ds(D, D // 2)], out_u.at[layer, pl.ds(0, D // 2), cols], outs.at[0, 2 + half]))
        if odd:
            rows = pl.ds(pl.multiple_of(j * C, C), C)
            made.append(pltpu.make_async_copy(OT.at[s], out_d.at[layer, rows, :], outs.at[1, 4]))
        return made

    def stage_d1(q, c):
        c("d1").start()

    def stage_first(q, c):
        c("d1").wait()
        ST1[q] = add(G[q, core, their_y], DD[q, their_y])
        c("y1").start()

        @pl.when(outer)
        def _():
            ST2[q] = add(G[q, core, low], DD[q, low])
            c("z2").start()

    def stage_z1(q, c):
        @pl.when(outer)
        def _():
            c("y1").wait_recv()
            ST3[q] = add(G[q, core, mine_y], DD[q, mine_y], YR[q])
            c("z1").start()

    def stage_m2(q, c):
        @pl.when(inner)
        def _():
            c("z2").wait_recv()
            ST2[q, pl.ds(0, Q)] = add(G[q, core, their_m], DD[q, their_m], ZR2[q, pl.ds(pl.multiple_of((1 - mi) * Q, 16), Q)])
            c("m2").start()

    def stage_x1(q, c):
        @pl.when(inner)
        def _():
            c("y1").wait_recv()
            c("z1").wait_recv()
            ST3[q] = add(G[q, core, mine_y], DD[q, mine_y], YR[q], ZR1[q])
            c("x1").start()

    def stage_y2(q, c):
        @pl.when(inner)
        def _():
            c("m2").wait_recv()
            ST2[q, pl.ds(Q, Q)] = add(G[q, core, mine_m], DD[q, mine_m], ZR2[q, pl.ds(pl.multiple_of(mi * Q, 16), Q)], MR[q])
            c("y2").start()

    def stage_f(q, c):
        @pl.when(inner)
        def _():
            c("x1").wait()
            G[q, core, mine_y] = add(ST3[q], XR[q])
            c("f1").start()
            c("f2").start()

    def stage_g(q, c):
        @pl.when(inner)
        def _():
            c("y2").wait()
            G[q, core, mine_m] = add(ST2[q, pl.ds(Q, Q)], YX[q])
            c("g1").start()
            c("g2").start()

    def stage_f2(q, c):
        @pl.when(outer)
        def _():
            c("f1").wait_recv()
            c("f2").start()

    def stage_g3(q, c):
        @pl.when(inner)
        def _():
            c("g1").wait_recv()
            c("g3").start()

    def stage_d2(q, c):
        c("f2").wait_recv()

        @pl.when(outer)
        def _():
            c("g2").wait_recv()
            c("g3").wait_recv()

        c("d2").start()

    def stage_end(q, c):
        c("d2").wait()
        for name in ("y1", "f2"):
            c(name).wait_send()

        @pl.when(outer)
        def _():
            for name in ("z2", "z1"):
                c(name).wait_send()

        @pl.when(inner)
        def _():
            for name in ("m2", "f1", "g1", "g2", "g3"):
                c(name).wait_send()

    STAGES = {
        0: (stage_d1,), 1: (stage_first,), 4: (stage_z1,), 5: (stage_m2,), 8: (stage_x1, stage_y2),
        11: (stage_f, stage_g), 14: (stage_f2, stage_g3), 17: (stage_d2,),
    }
    END = 18

    def finish(c, odd):
        q, s = lax.rem(c, NS), lax.rem(c // 2, 2)

        @pl.when(c >= 1)
        def _():
            for copy in out_copies(c - 1, not odd):
                copy.wait()

        stage_end(q, copies(q))
        if odd:
            for half in range(2):
                OT[s, pl.ds(half * 128, 128), :] = G[q, half, pl.ds(D // 2, D)].T
        for copy in out_copies(c, odd):
            copy.start()

    def tick(u, k):
        for when, stages in sorted(STAGES.items(), reverse=True):
            if when % 2 != k:
                continue
            c = u - 2 - when // 2

            @pl.when((c >= 0) & (c < PIECES))
            def _(c=c, stages=stages):
                q = lax.rem(c, NS)
                for stage in stages:
                    stage(q, copies(q))

        if END % 2 == k:
            c = u - 2 - END // 2
            for odd in (False, True):

                @pl.when((c >= 0) & (c < PIECES) & (lax.rem(c + 2, 2) == int(odd)))
                def _(odd=odd):
                    finish(c, odd)

    def tokens(s, layer, first):
        for b in range(2):
            rows = pl.ds(first + b * 512, 512)
            gu = dot(A[layer, rows], WGU[s])
            gate, up = gu[:, :C], gu[:, C:]
            dact = dot_nt(DY[rows], WD[s]).astype(BF16).astype(F32)
            sig = sigmoid(gate)
            silu = gate * sig
            ACT[rows] = (silu * up).astype(BF16)
            DGU[rows, pl.ds(0, C)] = (dact * up * (sig + silu * (1.0 - sig))).astype(BF16)
            DGU[rows, pl.ds(C, C)] = (dact * silu).astype(BF16)

    def switch():
        def block(b, _):
            rows = pl.ds(pl.multiple_of(b * 256, 256), 256)
            h = H[rows].astype(F32)
            da = DA[rows].astype(BF16).astype(F32)
            scale = lax.rsqrt(jnp.mean(h * h, -1, keepdims=True) + 1e-6)
            along = jnp.sum(da * h, -1, keepdims=True) * (1.0 / D)
            dh = (scale * (da - h * (scale * scale * along))).astype(BF16)
            new = add(DY[rows], dh)
            DY[rows] = new
            DYT[:, rows] = new.T
            return _

        lax.fori_loop(0, T // 256, block, None)

    def step(u, _):
        i = u // 2
        busy = i < N
        even, odd = busy & (lax.rem(u, 2) == 0), busy & (lax.rem(u, 2) == 1)
        s, layer = lax.rem(i, 2), jnp.maximum(L - 1 - i // PER, 0)
        first, second = lax.rem(2 * i, NS), lax.rem(2 * i + 1, NS)

        tick(u, 0)

        @pl.when(u == 2 * PER)
        def _():
            switch()

        @pl.when(even)
        def _():
            for copy in weights(i):
                copy.wait()

            @pl.when(i + 1 < N)
            def _():
                for copy in weights(i + 1):
                    copy.start()

            tokens(s, layer, 0)

        @pl.when(odd)
        def _():
            g = dot(AT[layer], DGU[...]).astype(BF16)
            for half in range(2):
                cols = slice(half * 128, half * 128 + 128)
                G[first, half, pl.ds(0, D)] = g[:, cols]
                cols = slice(C + half * 128, C + half * 128 + 128)
                G[first, half, pl.ds(D, D // 2)] = g[: D // 2, cols]
                G[second, half, pl.ds(0, D // 2)] = g[D // 2 :, cols]

        tick(u, 1)

        @pl.when(even)
        def _():
            tokens(s, layer, T // 2)

        def down():
            g = dot(DYT[...], ACT[...]).astype(BF16)
            for half in range(2):
                G[second, half, pl.ds(D // 2, D)] = g[:, half * 128 : half * 128 + 128]

        @pl.when(odd & (i < PER))
        def _():
            for b in range(2):
                rows = pl.ds(b * 1024, 1024)
                DA[rows] += dot_nt(DGU[rows], WGU[s])
            down()

        @pl.when(odd & (i >= PER))
        def _():
            down()

        return _

    lax.fori_loop(0, PIECES + 2 + END // 2 + 1, step, None)
    for copy in out_copies(PIECES - 1, True):
        copy.wait()


def gradients_of(x, dy, wg, wu, wd):
    vm, dma = pltpu.VMEM, pltpu.SemaphoreType.DMA
    return pl.pallas_call(
        step_kernel,
        out_shape=[jax.ShapeDtypeStruct(w.shape, BF16) for w in (wg, wu, wd)],
        in_specs=[pl.BlockSpec(memory_space=pl.ANY)] * 5,
        out_specs=[pl.BlockSpec(memory_space=pl.ANY)] * 3,
        scratch_shapes=[
            vm((L, T, D), BF16), vm((L, D, T), BF16), vm((T, D), BF16), vm((D, T), BF16), vm((T, D), BF16), vm((T, D), F32),
            vm((T, C), BF16), vm((T, 2 * C), BF16), vm((512, FF), BF16),
            vm((D, FF), BF16), vm((D, FF), BF16), vm((FF, D), BF16),
            vm((2, D, 2 * C), BF16), vm((2, C, D), BF16), vm((2, C, D), BF16),
            vm((NS, 2, R, 128), BF16), vm((NS, R, 128), BF16), vm((NS, Q, 128), BF16), vm((NS, Q, 128), BF16), vm((NS, Q, 128), BF16),
            vm((NS, 2 * Q, 128), BF16), vm((NS, Q, 128), BF16), vm((NS, Q, 128), BF16),
            vm((NS, Q, 128), BF16), vm((NS, 2 * Q, 128), BF16), vm((NS, Q, 128), BF16),
            dma((12,)), dma((2, 3)), dma((2, 5)), dma((13, NS)), dma((13, NS)),
        ],
        compiler_params=pltpu.CompilerParams(collective_id=0, has_side_effects=True, vmem_limit_bytes=67043328),
    )(x, dy, wg, wu, wd)


def adamw(w, m, v, g):
    m = 0.9 * m + 0.1 * g
    v = 0.95 * v + 0.05 * g * g
    step = m * lax.rsqrt(v + 1e-8) + 0.1 * w
    return (w - 0.02 * step).astype(BF16), m, v


def update_kernel(*refs):
    w, m, v, g, new_w, new_m, new_v = (refs[i : i + 3] for i in range(0, 21, 3))
    for k in range(3):
        new_w[k][...], new_m[k][...], new_v[k][...] = adamw(w[k][...].astype(F32), m[k][...], v[k][...], g[k][...].astype(F32))


def update(w, m, v, g):
    parts = 8
    blocks = [pl.BlockSpec((1, a.shape[1] // parts, a.shape[2]), lambda i: (i // parts, lax.rem(i, parts), 0)) for a in w]
    return pl.pallas_call(
        update_kernel,
        grid=(L * parts,),
        out_shape=[jax.ShapeDtypeStruct(a.shape, kind) for kind in (BF16, F32, F32) for a in w],
        in_specs=blocks * 4,
        out_specs=blocks * 3,
        compiler_params=pltpu.CompilerParams(vmem_limit_bytes=67043328),
    )(*w, *m, *v, *g)


def solution(mesh):
    def step(x, dy, *arrays):
        weights, m, v = (arrays[i : i + 3] for i in (0, 3, 6))
        gradients = gradients_of(x, dy, *weights)
        return tuple(update(weights, m, v, gradients))

    return jax.shard_map(
        step,
        mesh=mesh,
        in_specs=(P(("rep", "dp"), None, None),) * 2 + (P(None, None, None),) * 9,
        out_specs=(P("rep", None, None),) * 9,
        check_vma=False,
    )
```

```python
import jax
import jax.numpy as jnp
from jax import lax
from jax.experimental import pallas as pl
from jax.experimental.pallas import tpu as pltpu
from jax.sharding import PartitionSpec as P

NAMES = ("w_gate", "w_up", "w_down")
F32, BF16 = jnp.float32, jnp.bfloat16
T, D, FF, L = 2048, 640, 2048, 2
C = 256
PER = FF // C
N = L * PER
PIECES = 2 * N
NS = 12
R = 3 * D // 2
Q = R // 4
MESH = pl.DeviceIdType.MESH
NT = (((1,), (1,)), ((), ()))


def normed(h):
    wide = h.astype(F32)
    scale = lax.rsqrt(jnp.mean(wide**2, -1, keepdims=True) + 1e-6)
    return (wide * scale).astype(BF16)


def dot(a, b):
    return jnp.dot(a, b, preferred_element_type=F32)


def dot_nt(a, b):
    return lax.dot_general(a, b, NT, preferred_element_type=F32)


def sigmoid(a):
    return 0.5 * jnp.tanh(0.5 * a) + 0.5


def add(*terms):
    total = terms[0].astype(F32)
    for term in terms[1:]:
        total = total + term.astype(F32)
    return total.astype(BF16)


def step_kernel(
    x, dy, wg, wu, wd, md, out_g, out_u, out_d, WF, WU, WFD, H, DA,
    A, AT, DY, DYT, ACT, DGU, ACTF, WGU, WD, OT,
    G, DD, YR, ZR1, XR, ZR2, MR, YX, ST1, ST2, ST3,
    ld, ws, outs, sent, got, kept,
):
    rep, dp = lax.axis_index("rep"), lax.axis_index("dp")
    core, z, y = lax.rem(dp, 2), lax.rem(dp // 2, 4), dp // 8
    at = lambda y, z, core: (rep, (y * 4 + z) * 2 + core)
    zo = z + 1 - 2 * lax.rem(z, 2)
    partner, across, end, mid = at(y, z, 1 - core), at(1 - y, z, core), at(y, zo, core), at(y, 3 - z, core)
    inner = (z == 1) | (z == 2)
    outer = (z == 0) | (z == 3)
    mi = lax.rem(z + 1, 2)
    mine_y, their_y = pl.multiple_of(y * Q, 16), pl.multiple_of((1 - y) * Q, 16)
    mine_m, their_m = pl.multiple_of(2 * Q + mi * Q, 16), pl.multiple_of(2 * Q + (1 - mi) * Q, 16)
    mine_y, their_y, mine_m, their_m = (pl.ds(start, Q) for start in (mine_y, their_y, mine_m, their_m))
    low = pl.ds(2 * Q, 2 * Q)

    def loads():
        start, rest = pl.ds(0, 512), pl.ds(512, T - 512)
        pairs = [(x.at[0, start], H.at[start])]
        for k in range(4):
            cols = pl.ds(k * 512, 512)
            pairs += [(wg.at[0, :, cols], WF.at[:, cols]), (wu.at[0, :, cols], WU.at[:, cols])]
        pairs += [(wd.at[0], WFD), (dy.at[0], DY), (x.at[0, rest], H.at[rest])]
        return [pltpu.make_async_copy(s, d, ld.at[i]) for i, (s, d) in enumerate(pairs)]

    def weights(i):
        layer, j, s = L - 1 - i // PER, lax.rem(i, PER), lax.rem(i, 2)
        cols = pl.ds(pl.multiple_of(j * C, C), C)
        return [
            pltpu.make_async_copy(wg.at[layer, :, cols], WGU.at[s, :, pl.ds(0, C)], ws.at[s, 0]),
            pltpu.make_async_copy(wu.at[layer, :, cols], WGU.at[s, :, pl.ds(C, C)], ws.at[s, 1]),
            pltpu.make_async_copy(wd.at[layer, cols, :], WD.at[s], ws.at[s, 2]),
        ]

    arriving = loads()
    for copy in arriving + weights(0):
        copy.start()

    def keep(n):
        source, target = ((wd.at[1], H), (md.at[1], DA))[n]
        return pltpu.make_async_copy(source, target, kept.at[n])

    barrier = pltpu.get_barrier_semaphore()
    for device in (partner, across, end):
        pl.semaphore_signal(barrier, inc=1, device_id=device, device_id_type=MESH)

    @pl.when(inner)
    def _():
        pl.semaphore_signal(barrier, inc=1, device_id=mid, device_id_type=MESH)

    def forward(rows, wait):
        wait(0, 1)
        x = H[rows]
        a = normed(x)
        A[0, rows] = a
        AT[0, :, rows] = a.T
        for k in range(4):
            wait(2 * k + 1, 2 * k + 3)
            cols = pl.ds(k * 512, 512)
            gate, up = dot(a, WF[:, cols]), dot(a, WU[:, cols])
            ACTF[:, cols] = (gate * sigmoid(gate) * up).astype(BF16)
        wait(9, 11)
        DYT[:, rows] = DY[rows].T
        DA[rows] = jnp.zeros((512, D), F32)
        h = add(x, dot(ACTF[...], WFD[...]).astype(BF16))
        H[rows] = h
        a = normed(h)
        A[1, rows] = a
        AT[1, :, rows] = a.T

    def now(first, last):
        for copy in arriving[first:last]:
            copy.wait()

    def later(b, _):
        forward(pl.ds(pl.multiple_of(b * 512, 512), 512), lambda first, last: None)
        return _

    forward(pl.ds(0, 512), now)
    now(11, 12)
    lax.fori_loop(1, T // 512, later, None)
    pl.semaphore_wait(barrier, 3 + inner.astype(jnp.int32))

    def copies(q):
        def remote(n, src, dst, device):
            return pltpu.make_async_remote_copy(
                src_ref=src, dst_ref=dst, send_sem=sent.at[n, q], recv_sem=got.at[n, q], device_id=device, device_id_type=MESH
            )

        own = G.at[q, core]
        made = dict(
            d1=lambda: remote(0, G.at[q, 1 - core], DD.at[q], partner),
            y1=lambda: remote(1, ST1.at[q], YR.at[q], across),
            z2=lambda: remote(2, ST2.at[q], ZR2.at[q], end),
            z1=lambda: remote(3, ST3.at[q], ZR1.at[q], end),
            m2=lambda: remote(4, ST2.at[q, pl.ds(0, Q)], MR.at[q], mid),
            x1=lambda: remote(5, ST3.at[q], XR.at[q], mid),
            y2=lambda: remote(6, ST2.at[q, pl.ds(Q, Q)], YX.at[q], across),
            f1=lambda: remote(7, own.at[mine_y], own.at[mine_y], end),
            f2=lambda: remote(8, own.at[mine_y], own.at[mine_y], across),
            g1=lambda: remote(9, own.at[mine_m], own.at[mine_m], mid),
            g2=lambda: remote(10, own.at[mine_m], own.at[mine_m], end),
            g3=lambda: remote(11, own.at[their_m], own.at[their_m], end),
            d2=lambda: remote(12, own, own, partner),
        )
        return lambda name: made[name]()

    def out_copies(c, odd):
        layer, j, q, s = L - 1 - c // (2 * PER), lax.rem(c // 2, PER), lax.rem(c, NS), lax.rem(c // 2, 2)
        made = []
        for half in range(2):
            cols = pl.ds(pl.multiple_of(j * C + half * 128, 128), 128)
            if odd:
                made.append(pltpu.make_async_copy(G.at[q, half, pl.ds(0, D // 2)], out_u.at[layer, pl.ds(D // 2, D // 2), cols], outs.at[1, half]))
            else:
                made.append(pltpu.make_async_copy(G.at[q, half, pl.ds(0, D)], out_g.at[layer, :, cols], outs.at[0, half]))
                made.append(pltpu.make_async_copy(G.at[q, half, pl.ds(D, D // 2)], out_u.at[layer, pl.ds(0, D // 2), cols], outs.at[0, 2 + half]))
        if odd:
            rows = pl.ds(pl.multiple_of(j * C, C), C)
            made.append(pltpu.make_async_copy(OT.at[s], out_d.at[layer, rows, :], outs.at[1, 4]))
        return made

    def stage_d1(q, c):
        c("d1").start()

    def stage_first(q, c):
        c("d1").wait()
        ST1[q] = add(G[q, core, their_y], DD[q, their_y])
        c("y1").start()

        @pl.when(outer)
        def _():
            ST2[q] = add(G[q, core, low], DD[q, low])
            c("z2").start()

    def stage_z1(q, c):
        @pl.when(outer)
        def _():
            c("y1").wait_recv()
            ST3[q] = add(G[q, core, mine_y], DD[q, mine_y], YR[q])
            c("z1").start()

    def stage_m2(q, c):
        @pl.when(inner)
        def _():
            c("z2").wait_recv()
            ST2[q, pl.ds(0, Q)] = add(G[q, core, their_m], DD[q, their_m], ZR2[q, pl.ds(pl.multiple_of((1 - mi) * Q, 16), Q)])
            c("m2").start()

    def stage_x1(q, c):
        @pl.when(inner)
        def _():
            c("y1").wait_recv()
            c("z1").wait_recv()
            ST3[q] = add(G[q, core, mine_y], DD[q, mine_y], YR[q], ZR1[q])
            c("x1").start()

    def stage_y2(q, c):
        @pl.when(inner)
        def _():
            c("m2").wait_recv()
            ST2[q, pl.ds(Q, Q)] = add(G[q, core, mine_m], DD[q, mine_m], ZR2[q, pl.ds(pl.multiple_of(mi * Q, 16), Q)], MR[q])
            c("y2").start()

    def stage_f(q, c):
        @pl.when(inner)
        def _():
            c("x1").wait()
            G[q, core, mine_y] = add(ST3[q], XR[q])
            c("f1").start()
            c("f2").start()

    def stage_g(q, c):
        @pl.when(inner)
        def _():
            c("y2").wait()
            G[q, core, mine_m] = add(ST2[q, pl.ds(Q, Q)], YX[q])
            c("g1").start()
            c("g2").start()

    def stage_f2(q, c):
        @pl.when(outer)
        def _():
            c("f1").wait_recv()
            c("f2").start()

    def stage_g3(q, c):
        @pl.when(inner)
        def _():
            c("g1").wait_recv()
            c("g3").start()

    def stage_d2(q, c):
        c("f2").wait_recv()

        @pl.when(outer)
        def _():
            c("g2").wait_recv()
            c("g3").wait_recv()

        c("d2").start()

    def stage_end(q, c):
        c("d2").wait()
        for name in ("y1", "f2"):
            c(name).wait_send()

        @pl.when(outer)
        def _():
            for name in ("z2", "z1"):
                c(name).wait_send()

        @pl.when(inner)
        def _():
            for name in ("m2", "f1", "g1", "g2", "g3"):
                c(name).wait_send()

    STAGES = {
        0: (stage_d1,), 1: (stage_first,), 3: (stage_z1,), 5: (stage_m2,), 6: (stage_x1,), 8: (stage_y2,),
        9: (stage_f,), 11: (stage_g,), 12: (stage_f2,), 14: (stage_g3,), 17: (stage_d2,),
    }
    END = 18

    def finish(c, odd):
        q, s = lax.rem(c, NS), lax.rem(c // 2, 2)

        @pl.when(c >= 1)
        def _():
            for copy in out_copies(c - 1, not odd):
                copy.wait()

        stage_end(q, copies(q))
        if odd:
            for half in range(2):
                OT[s, pl.ds(half * 128, 128), :] = G[q, half, pl.ds(D // 2, D)].T
        for copy in out_copies(c, odd):
            copy.start()

    def tick(u, k):
        for when, stages in sorted(STAGES.items(), reverse=True):
            if when % 2 != k:
                continue
            c = u - 2 - when // 2

            @pl.when((c >= 0) & (c < PIECES))
            def _(c=c, stages=stages):
                q = lax.rem(c, NS)
                for stage in stages:
                    stage(q, copies(q))

        if END % 2 == k:
            c = u - 2 - END // 2
            for odd in (False, True):

                @pl.when((c >= 0) & (c < PIECES) & (lax.rem(c + 2, 2) == int(odd)))
                def _(odd=odd):
                    finish(c, odd)

    def tokens(s, layer, first):
        for b in range(2):
            rows = pl.ds(first + b * 512, 512)
            gu = dot(A[layer, rows], WGU[s])
            gate, up = gu[:, :C], gu[:, C:]
            dact = dot_nt(DY[rows], WD[s]).astype(BF16).astype(F32)
            sig = sigmoid(gate)
            silu = gate * sig
            ACT[rows] = (silu * up).astype(BF16)
            DGU[rows, pl.ds(0, C)] = (dact * up * (sig + silu * (1.0 - sig))).astype(BF16)
            DGU[rows, pl.ds(C, C)] = (dact * silu).astype(BF16)

    def switch():
        def block(b, _):
            rows = pl.ds(pl.multiple_of(b * 256, 256), 256)
            h = H[rows].astype(F32)
            da = DA[rows].astype(BF16).astype(F32)
            scale = lax.rsqrt(jnp.mean(h * h, -1, keepdims=True) + 1e-6)
            along = jnp.sum(da * h, -1, keepdims=True) * (1.0 / D)
            dh = (scale * (da - h * (scale * scale * along))).astype(BF16)
            new = add(DY[rows], dh)
            DY[rows] = new
            DYT[:, rows] = new.T
            return _

        lax.fori_loop(0, T // 256, block, None)

    def step(u, _):
        i = u // 2
        busy = i < N
        even, odd = busy & (lax.rem(u, 2) == 0), busy & (lax.rem(u, 2) == 1)
        s, layer = lax.rem(i, 2), jnp.maximum(L - 1 - i // PER, 0)
        first, second = lax.rem(2 * i, NS), lax.rem(2 * i + 1, NS)

        tick(u, 0)

        @pl.when(u == 2 * PER)
        def _():
            switch()
            for n in range(2):
                keep(n).start()

        @pl.when(even)
        def _():
            for copy in weights(i):
                copy.wait()

            @pl.when(i + 1 < N)
            def _():
                for copy in weights(i + 1):
                    copy.start()

            tokens(s, layer, 0)

        @pl.when(odd)
        def _():
            g = dot(AT[layer], DGU[...]).astype(BF16)
            for half in range(2):
                cols = slice(half * 128, half * 128 + 128)
                G[first, half, pl.ds(0, D)] = g[:, cols]
                cols = slice(C + half * 128, C + half * 128 + 128)
                G[first, half, pl.ds(D, D // 2)] = g[: D // 2, cols]
                G[second, half, pl.ds(0, D // 2)] = g[D // 2 :, cols]

        tick(u, 1)

        @pl.when(even)
        def _():
            tokens(s, layer, T // 2)

        def down():
            g = dot(DYT[...], ACT[...]).astype(BF16)
            for half in range(2):
                G[second, half, pl.ds(D // 2, D)] = g[:, half * 128 : half * 128 + 128]

        @pl.when(odd & (i < PER))
        def _():
            for b in range(2):
                rows = pl.ds(b * 1024, 1024)
                DA[rows] += dot_nt(DGU[rows], WGU[s])
            down()

        @pl.when(odd & (i >= PER))
        def _():
            down()

        return _

    lax.fori_loop(0, PIECES + 2 + END // 2 + 1, step, None)
    for copy in out_copies(PIECES - 1, True) + [keep(n) for n in range(2)]:
        copy.wait()


def gradients_of(x, dy, wg, wu, wd, md):
    vm, dma = pltpu.VMEM, pltpu.SemaphoreType.DMA
    return pl.pallas_call(
        step_kernel,
        out_shape=[jax.ShapeDtypeStruct(w.shape, BF16) for w in (wg, wu, wd)]
        + [vm((D, FF), BF16), vm((D, FF), BF16), vm((FF, D), BF16), vm((T, D), BF16), vm((T, D), F32)],
        in_specs=[pl.BlockSpec(memory_space=pl.ANY)] * 6,
        out_specs=[pl.BlockSpec(memory_space=pl.ANY)] * 3 + [pl.BlockSpec(memory_space=vm)] * 5,
        scratch_shapes=[
            vm((L, T, D), BF16), vm((L, D, T), BF16), vm((T, D), BF16), vm((D, T), BF16),
            vm((T, C), BF16), vm((T, 2 * C), BF16), vm((512, FF), BF16),
            vm((2, D, 2 * C), BF16), vm((2, C, D), BF16), vm((2, C, D), BF16),
            vm((NS, 2, R, 128), BF16), vm((NS, R, 128), BF16), vm((NS, Q, 128), BF16), vm((NS, Q, 128), BF16), vm((NS, Q, 128), BF16),
            vm((NS, 2 * Q, 128), BF16), vm((NS, Q, 128), BF16), vm((NS, Q, 128), BF16),
            vm((NS, Q, 128), BF16), vm((NS, 2 * Q, 128), BF16), vm((NS, Q, 128), BF16),
            dma((12,)), dma((2, 3)), dma((2, 5)), dma((13, NS)), dma((13, NS)), dma((2,)),
        ],
        compiler_params=pltpu.CompilerParams(collective_id=0, has_side_effects=True, vmem_limit_bytes=51 * 10**6),
    )(x, dy, wg, wu, wd, md)


def adamw(w, m, v, g):
    m = 0.9 * m + 0.1 * g
    v = 0.95 * v + 0.05 * g * g
    step = m * lax.rsqrt(v + 1e-8) + 0.1 * w
    return (w - 0.02 * step).astype(BF16), m, v


PARTS = 8


def update_kernel(*refs):
    w0, (w1_down, m1_down), w1 = refs[0:3], refs[3:5], refs[5:7]
    m, v, g, new_w, new_m, new_v = (refs[i : i + 3] for i in range(7, 25, 3))
    layer, part = pl.program_id(0) // PARTS, lax.rem(pl.program_id(0), PARTS)
    wide = pl.ds(pl.multiple_of(part * (D // PARTS), D // PARTS), D // PARTS)
    tall = pl.ds(pl.multiple_of(part * (FF // PARTS), FF // PARTS), FF // PARTS)

    def step(w, old_m):
        for k in range(3):
            new_w[k][0], new_m[k][0], new_v[k][0] = adamw(w[k].astype(F32), old_m[k], v[k][0], g[k][0].astype(F32))

    @pl.when(layer == 0)
    def _():
        step((w0[0][wide], w0[1][wide], w0[2][tall]), (m[0][0], m[1][0], m[2][0]))

    @pl.when(layer == 1)
    def _():
        step((w1[0][0], w1[1][0], w1_down[tall]), (m[0][0], m[1][0], m1_down[tall]))


def update(kept, w, m, v, g):
    blocks = [pl.BlockSpec((1, a.shape[1] // PARTS, a.shape[2]), lambda i: (i // PARTS, lax.rem(i, PARTS), 0)) for a in m]
    first = pl.BlockSpec((1, FF // PARTS, D), lambda i: (0, jnp.minimum(i, PARTS - 1), 0))
    second = pl.BlockSpec((1, D // PARTS, FF), lambda i: (1, jnp.maximum(i - PARTS, 0), 0))
    return pl.pallas_call(
        update_kernel,
        grid=(L * PARTS,),
        out_shape=[jax.ShapeDtypeStruct(a.shape, kind) for kind in (BF16, F32, F32) for a in m],
        in_specs=[pl.BlockSpec(memory_space=pltpu.VMEM)] * 5 + [second] * 2 + blocks[:2] + [first] + blocks * 2,
        out_specs=blocks * 3,
        compiler_params=pltpu.CompilerParams(vmem_limit_bytes=38 * 10**6),
    )(*kept, *w[:2], *m, *v, *g)


def solution(mesh):
    def step(x, dy, *arrays):
        weights, m, v = (arrays[i : i + 3] for i in (0, 3, 6))
        gathered = gradients_of(x, dy, *weights, m[2])
        return tuple(update(gathered[3:], weights, m, v, gathered[:3]))

    return jax.shard_map(
        step,
        mesh=mesh,
        in_specs=(P(("rep", "dp"), None, None),) * 2 + (P(None, None, None),) * 9,
        out_specs=(P("rep", None, None),) * 9,
        check_vma=False,
    )
```

```python
import jax
import jax.numpy as jnp
from jax import lax
from jax.experimental import pallas as pl
from jax.experimental.pallas import tpu as pltpu
from jax.sharding import PartitionSpec as P

NAMES = ("w_gate", "w_up", "w_down")
F32, BF16 = jnp.float32, jnp.bfloat16
T, D, FF, L = 2048, 640, 2048, 2
C = 256
PER = FF // C
N = L * PER
PIECES = 2 * N
NS = 12
R = 3 * D // 2
Q = R // 4
MESH = pl.DeviceIdType.MESH
NT = (((1,), (1,)), ((), ()))


def normed(h):
    wide = h.astype(F32)
    scale = lax.rsqrt(jnp.mean(wide**2, -1, keepdims=True) + 1e-6)
    return (wide * scale).astype(BF16)


def dot(a, b):
    return jnp.dot(a, b, preferred_element_type=F32)


def dot_nt(a, b):
    return lax.dot_general(a, b, NT, preferred_element_type=F32)


def sigmoid(a):
    return 0.5 * jnp.tanh(0.5 * a) + 0.5


def add(*terms):
    total = terms[0].astype(F32)
    for term in terms[1:]:
        total = total + term.astype(F32)
    return total.astype(BF16)


def step_kernel(
    x, dy, wg, wu, wd, md, out_g, out_u, out_d, WF, WU, WFD, H, DA,
    A, AT, DY, DYT, ACT, DGU, ACTF, WGU, WD, OT,
    G, DD, YR, ZR1, XR, ZR2, MR, YX, ST1, ST2, ST3,
    ld, ws, outs, sent, got, kept,
):
    rep, dp = lax.axis_index("rep"), lax.axis_index("dp")
    core, z, y = lax.rem(dp, 2), lax.rem(dp // 2, 4), dp // 8
    at = lambda y, z, core: (rep, (y * 4 + z) * 2 + core)
    zo = z + 1 - 2 * lax.rem(z, 2)
    partner, across, end, mid = at(y, z, 1 - core), at(1 - y, z, core), at(y, zo, core), at(y, 3 - z, core)
    inner = (z == 1) | (z == 2)
    outer = (z == 0) | (z == 3)
    mi = lax.rem(z + 1, 2)
    mine_y, their_y = pl.multiple_of(y * Q, 16), pl.multiple_of((1 - y) * Q, 16)
    mine_m, their_m = pl.multiple_of(2 * Q + mi * Q, 16), pl.multiple_of(2 * Q + (1 - mi) * Q, 16)
    mine_y, their_y, mine_m, their_m = (pl.ds(start, Q) for start in (mine_y, their_y, mine_m, their_m))
    low = pl.ds(2 * Q, 2 * Q)

    def loads():
        start, rest = pl.ds(0, 512), pl.ds(512, T - 512)
        pairs = [(x.at[0, start], H.at[start])]
        for k in range(4):
            cols = pl.ds(k * 512, 512)
            pairs += [(wg.at[0, :, cols], WF.at[:, cols]), (wu.at[0, :, cols], WU.at[:, cols])]
        pairs += [(wd.at[0], WFD), (dy.at[0], DY), (x.at[0, rest], H.at[rest])]
        return [pltpu.make_async_copy(s, d, ld.at[i]) for i, (s, d) in enumerate(pairs)]

    def weights(i):
        layer, j, s = L - 1 - i // PER, lax.rem(i, PER), lax.rem(i, 2)
        cols = pl.ds(pl.multiple_of(j * C, C), C)
        return [
            pltpu.make_async_copy(wg.at[layer, :, cols], WGU.at[s, :, pl.ds(0, C)], ws.at[s, 0]),
            pltpu.make_async_copy(wu.at[layer, :, cols], WGU.at[s, :, pl.ds(C, C)], ws.at[s, 1]),
            pltpu.make_async_copy(wd.at[layer, cols, :], WD.at[s], ws.at[s, 2]),
        ]

    arriving = loads()
    for copy in arriving + weights(0):
        copy.start()

    def keep(n):
        source, target = ((wd.at[1], H), (md.at[1], DA))[n]
        return pltpu.make_async_copy(source, target, kept.at[n])

    barrier = pltpu.get_barrier_semaphore()
    for device in (partner, across, end):
        pl.semaphore_signal(barrier, inc=1, device_id=device, device_id_type=MESH)

    @pl.when(inner)
    def _():
        pl.semaphore_signal(barrier, inc=1, device_id=mid, device_id_type=MESH)

    def forward(rows, wait):
        wait(0, 1)
        x = H[rows]
        a = normed(x)
        A[0, rows] = a
        AT[0, :, rows] = a.T
        for k in range(4):
            wait(2 * k + 1, 2 * k + 3)
            cols = pl.ds(k * 512, 512)
            gate, up = dot(a, WF[:, cols]), dot(a, WU[:, cols])
            ACTF[:, cols] = (gate * sigmoid(gate) * up).astype(BF16)
        wait(9, 11)
        DYT[:, rows] = DY[rows].T
        DA[rows] = jnp.zeros((512, D), F32)
        h = add(x, dot(ACTF[...], WFD[...]).astype(BF16))
        H[rows] = h
        a = normed(h)
        A[1, rows] = a
        AT[1, :, rows] = a.T

    def now(first, last):
        for copy in arriving[first:last]:
            copy.wait()

    def later(b, _):
        forward(pl.ds(pl.multiple_of(b * 512, 512), 512), lambda first, last: None)
        return _

    forward(pl.ds(0, 512), now)
    now(11, 12)
    lax.fori_loop(1, T // 512, later, None)
    pl.semaphore_wait(barrier, 3 + inner.astype(jnp.int32))

    def copies(q):
        def remote(n, src, dst, device):
            return pltpu.make_async_remote_copy(
                src_ref=src, dst_ref=dst, send_sem=sent.at[n, q], recv_sem=got.at[n, q], device_id=device, device_id_type=MESH
            )

        own = G.at[q, core]
        made = dict(
            d1=lambda: remote(0, G.at[q, 1 - core], DD.at[q], partner),
            y1=lambda: remote(1, ST1.at[q], YR.at[q], across),
            z2=lambda: remote(2, ST2.at[q], ZR2.at[q], end),
            z1=lambda: remote(3, ST3.at[q], ZR1.at[q], end),
            m2=lambda: remote(4, ST2.at[q, pl.ds(0, Q)], MR.at[q], mid),
            x1=lambda: remote(5, ST3.at[q], XR.at[q], mid),
            y2=lambda: remote(6, ST2.at[q, pl.ds(Q, Q)], YX.at[q], across),
            f1=lambda: remote(7, own.at[mine_y], own.at[mine_y], end),
            f2=lambda: remote(8, own.at[mine_y], own.at[mine_y], across),
            g1=lambda: remote(9, own.at[mine_m], own.at[mine_m], mid),
            g2=lambda: remote(10, own.at[mine_m], own.at[mine_m], end),
            g3=lambda: remote(11, own.at[their_m], own.at[their_m], end),
            d2=lambda: remote(12, own, own, partner),
        )
        return lambda name: made[name]()

    def out_copies(c, odd):
        layer, j, q, s = L - 1 - c // (2 * PER), lax.rem(c // 2, PER), lax.rem(c, NS), lax.rem(c // 2, 2)
        made = []
        for half in range(2):
            cols = pl.ds(pl.multiple_of(j * C + half * 128, 128), 128)
            if odd:
                made.append(pltpu.make_async_copy(G.at[q, half, pl.ds(0, D // 2)], out_u.at[layer, pl.ds(D // 2, D // 2), cols], outs.at[1, half]))
            else:
                made.append(pltpu.make_async_copy(G.at[q, half, pl.ds(0, D)], out_g.at[layer, :, cols], outs.at[0, half]))
                made.append(pltpu.make_async_copy(G.at[q, half, pl.ds(D, D // 2)], out_u.at[layer, pl.ds(0, D // 2), cols], outs.at[0, 2 + half]))
        if odd:
            rows = pl.ds(pl.multiple_of(j * C, C), C)
            made.append(pltpu.make_async_copy(OT.at[s], out_d.at[layer, rows, :], outs.at[1, 4]))
        return made

    def stage_d1(q, c):
        c("d1").start()

    def stage_first(q, c):
        c("d1").wait()
        ST1[q] = add(G[q, core, their_y], DD[q, their_y])
        c("y1").start()

        @pl.when(outer)
        def _():
            ST2[q] = add(G[q, core, low], DD[q, low])
            c("z2").start()

    def stage_z1(q, c):
        @pl.when(outer)
        def _():
            c("y1").wait_recv()
            ST3[q] = add(G[q, core, mine_y], DD[q, mine_y], YR[q])
            c("z1").start()

    def stage_m2(q, c):
        @pl.when(inner)
        def _():
            c("z2").wait_recv()
            ST2[q, pl.ds(0, Q)] = add(G[q, core, their_m], DD[q, their_m], ZR2[q, pl.ds(pl.multiple_of((1 - mi) * Q, 16), Q)])
            c("m2").start()

    def stage_x1(q, c):
        @pl.when(inner)
        def _():
            c("y1").wait_recv()
            c("z1").wait_recv()
            ST3[q] = add(G[q, core, mine_y], DD[q, mine_y], YR[q], ZR1[q])
            c("x1").start()

    def stage_y2(q, c):
        @pl.when(inner)
        def _():
            c("m2").wait_recv()
            ST2[q, pl.ds(Q, Q)] = add(G[q, core, mine_m], DD[q, mine_m], ZR2[q, pl.ds(pl.multiple_of(mi * Q, 16), Q)], MR[q])
            c("y2").start()

    def stage_f(q, c):
        @pl.when(inner)
        def _():
            c("x1").wait()
            G[q, core, mine_y] = add(ST3[q], XR[q])
            c("f1").start()
            c("f2").start()

    def stage_g(q, c):
        @pl.when(inner)
        def _():
            c("y2").wait()
            G[q, core, mine_m] = add(ST2[q, pl.ds(Q, Q)], YX[q])
            c("g1").start()
            c("g2").start()

    def stage_f2(q, c):
        @pl.when(outer)
        def _():
            c("f1").wait_recv()
            c("f2").start()

    def stage_g3(q, c):
        @pl.when(inner)
        def _():
            c("g1").wait_recv()
            c("g3").start()

    def stage_d2(q, c):
        c("f2").wait_recv()

        @pl.when(outer)
        def _():
            c("g2").wait_recv()
            c("g3").wait_recv()

        c("d2").start()

    def stage_end(q, c):
        c("d2").wait()
        for name in ("y1", "f2"):
            c(name).wait_send()

        @pl.when(outer)
        def _():
            for name in ("z2", "z1"):
                c(name).wait_send()

        @pl.when(inner)
        def _():
            for name in ("m2", "f1", "g1", "g2", "g3"):
                c(name).wait_send()

    STAGES = {
        0: (stage_d1,), 1: (stage_first,), 3: (stage_z1,), 5: (stage_m2,), 6: (stage_x1,), 8: (stage_y2,),
        9: (stage_f,), 11: (stage_g,), 12: (stage_f2,), 14: (stage_g3,), 17: (stage_d2,),
    }
    END = 18

    def finish(c, odd):
        q, s = lax.rem(c, NS), lax.rem(c // 2, 2)

        @pl.when(c >= 1)
        def _():
            for copy in out_copies(c - 1, not odd):
                copy.wait()

        stage_end(q, copies(q))
        if odd:
            for half in range(2):
                OT[s, pl.ds(half * 128, 128), :] = G[q, half, pl.ds(D // 2, D)].T
        for copy in out_copies(c, odd):
            copy.start()

    def tick(u, k):
        for when, stages in sorted(STAGES.items(), reverse=True):
            if when % 2 == k:
                continue
            c = u - (when + 3 - k) // 2

            @pl.when((c >= 0) & (c < PIECES))
            def _(c=c, stages=stages):
                q = lax.rem(c, NS)
                for stage in stages:
                    stage(q, copies(q))

        if END % 2 != k:
            c = u - (END + 3 - k) // 2
            for odd in (False, True):

                @pl.when((c >= 0) & (c < PIECES) & (lax.rem(c + 2, 2) == int(odd)))
                def _(odd=odd):
                    finish(c, odd)

    def tokens(s, layer, first):
        for b in range(2):
            rows = pl.ds(first + b * 512, 512)
            gu = dot(A[layer, rows], WGU[s])
            gate, up = gu[:, :C], gu[:, C:]
            dact = dot_nt(DY[rows], WD[s]).astype(BF16).astype(F32)
            sig = sigmoid(gate)
            silu = gate * sig
            ACT[rows] = (silu * up).astype(BF16)
            DGU[rows, pl.ds(0, C)] = (dact * up * (sig + silu * (1.0 - sig))).astype(BF16)
            DGU[rows, pl.ds(C, C)] = (dact * silu).astype(BF16)

    def switch():
        def block(b, _):
            rows = pl.ds(pl.multiple_of(b * 256, 256), 256)
            h = H[rows].astype(F32)
            da = DA[rows].astype(BF16).astype(F32)
            scale = lax.rsqrt(jnp.mean(h * h, -1, keepdims=True) + 1e-6)
            along = jnp.sum(da * h, -1, keepdims=True) * (1.0 / D)
            dh = (scale * (da - h * (scale * scale * along))).astype(BF16)
            new = add(DY[rows], dh)
            DY[rows] = new
            DYT[:, rows] = new.T
            return _

        lax.fori_loop(0, T // 256, block, None)

    def step(u, _):
        i = u // 2
        busy = i < N
        even, odd = busy & (lax.rem(u, 2) == 0), busy & (lax.rem(u, 2) == 1)
        s, layer = lax.rem(i, 2), jnp.maximum(L - 1 - i // PER, 0)
        first, second = lax.rem(2 * i, NS), lax.rem(2 * i + 1, NS)

        tick(u, 0)

        @pl.when(u == 2 * PER)
        def _():
            switch()
            for n in range(2):
                keep(n).start()

        @pl.when(even)
        def _():
            for copy in weights(i):
                copy.wait()

            @pl.when(i + 1 < N)
            def _():
                for copy in weights(i + 1):
                    copy.start()

            tokens(s, layer, 0)

        @pl.when(odd)
        def _():
            g = dot(AT[layer], DGU[...]).astype(BF16)
            for half in range(2):
                cols = slice(half * 128, half * 128 + 128)
                G[first, half, pl.ds(0, D)] = g[:, cols]
                cols = slice(C + half * 128, C + half * 128 + 128)
                G[first, half, pl.ds(D, D // 2)] = g[: D // 2, cols]
                G[second, half, pl.ds(0, D // 2)] = g[D // 2 :, cols]

        tick(u, 1)

        @pl.when(even)
        def _():
            tokens(s, layer, T // 2)

        def down():
            g = dot(DYT[...], ACT[...]).astype(BF16)
            for half in range(2):
                G[second, half, pl.ds(D // 2, D)] = g[:, half * 128 : half * 128 + 128]

        @pl.when(odd & (i < PER))
        def _():
            for b in range(2):
                rows = pl.ds(b * 1024, 1024)
                DA[rows] += dot_nt(DGU[rows], WGU[s])
            down()

        @pl.when(odd & (i >= PER))
        def _():
            down()

        return _

    lax.fori_loop(0, PIECES + (END + 2) // 2, step, None)
    for copy in out_copies(PIECES - 1, True) + [keep(n) for n in range(2)]:
        copy.wait()


def gradients_of(x, dy, wg, wu, wd, md):
    vm, dma = pltpu.VMEM, pltpu.SemaphoreType.DMA
    return pl.pallas_call(
        step_kernel,
        out_shape=[jax.ShapeDtypeStruct(w.shape, BF16) for w in (wg, wu, wd)]
        + [vm((D, FF), BF16), vm((D, FF), BF16), vm((FF, D), BF16), vm((T, D), BF16), vm((T, D), F32)],
        in_specs=[pl.BlockSpec(memory_space=pl.ANY)] * 6,
        out_specs=[pl.BlockSpec(memory_space=pl.ANY)] * 3 + [pl.BlockSpec(memory_space=vm)] * 5,
        scratch_shapes=[
            vm((L, T, D), BF16), vm((L, D, T), BF16), vm((T, D), BF16), vm((D, T), BF16),
            vm((T, C), BF16), vm((T, 2 * C), BF16), vm((512, FF), BF16),
            vm((2, D, 2 * C), BF16), vm((2, C, D), BF16), vm((2, C, D), BF16),
            vm((NS, 2, R, 128), BF16), vm((NS, R, 128), BF16), vm((NS, Q, 128), BF16), vm((NS, Q, 128), BF16), vm((NS, Q, 128), BF16),
            vm((NS, 2 * Q, 128), BF16), vm((NS, Q, 128), BF16), vm((NS, Q, 128), BF16),
            vm((NS, Q, 128), BF16), vm((NS, 2 * Q, 128), BF16), vm((NS, Q, 128), BF16),
            dma((12,)), dma((2, 3)), dma((2, 5)), dma((13, NS)), dma((13, NS)), dma((2,)),
        ],
        compiler_params=pltpu.CompilerParams(collective_id=0, has_side_effects=True, vmem_limit_bytes=51 * 10**6),
    )(x, dy, wg, wu, wd, md)


def adamw(w, m, v, g):
    m = 0.9 * m + 0.1 * g
    v = 0.95 * v + 0.05 * g * g
    step = m * lax.rsqrt(v + 1e-8) + 0.1 * w
    return (w - 0.02 * step).astype(BF16), m, v


PARTS = 8


def update_kernel(*refs):
    w0, (w1_down, m1_down), w1 = refs[0:3], refs[3:5], refs[5:7]
    m, v, g, new_w, new_m, new_v = (refs[i : i + 3] for i in range(7, 25, 3))
    layer, part = pl.program_id(0) // PARTS, lax.rem(pl.program_id(0), PARTS)
    wide = pl.ds(pl.multiple_of(part * (D // PARTS), D // PARTS), D // PARTS)
    tall = pl.ds(pl.multiple_of(part * (FF // PARTS), FF // PARTS), FF // PARTS)

    def step(w, old_m):
        for k in range(3):
            new_w[k][0], new_m[k][0], new_v[k][0] = adamw(w[k].astype(F32), old_m[k], v[k][0], g[k][0].astype(F32))

    @pl.when(layer == 0)
    def _():
        step((w0[0][wide], w0[1][wide], w0[2][tall]), (m[0][0], m[1][0], m[2][0]))

    @pl.when(layer == 1)
    def _():
        step((w1[0][0], w1[1][0], w1_down[tall]), (m[0][0], m[1][0], m1_down[tall]))


def update(kept, w, m, v, g):
    blocks = [pl.BlockSpec((1, a.shape[1] // PARTS, a.shape[2]), lambda i: (i // PARTS, lax.rem(i, PARTS), 0)) for a in m]
    first = pl.BlockSpec((1, FF // PARTS, D), lambda i: (0, jnp.minimum(i, PARTS - 1), 0))
    second = pl.BlockSpec((1, D // PARTS, FF), lambda i: (1, jnp.maximum(i - PARTS, 0), 0))
    return pl.pallas_call(
        update_kernel,
        grid=(L * PARTS,),
        out_shape=[jax.ShapeDtypeStruct(a.shape, kind) for kind in (BF16, F32, F32) for a in m],
        in_specs=[pl.BlockSpec(memory_space=pltpu.VMEM)] * 5 + [second] * 2 + blocks[:2] + [first] + blocks * 2,
        out_specs=blocks * 3,
        compiler_params=pltpu.CompilerParams(vmem_limit_bytes=38 * 10**6),
    )(*kept, *w[:2], *m, *v, *g)


def solution(mesh):
    def step(x, dy, *arrays):
        weights, m, v = (arrays[i : i + 3] for i in (0, 3, 6))
        gathered = gradients_of(x, dy, *weights, m[2])
        return tuple(update(gathered[3:], weights, m, v, gathered[:3]))

    return jax.shard_map(
        step,
        mesh=mesh,
        in_specs=(P(("rep", "dp"), None, None),) * 2 + (P(None, None, None),) * 9,
        out_specs=(P("rep", None, None),) * 9,
        check_vma=False,
    )
```
